32 devices in a mesh: req: 8 (over y, x, core), kv: 4 (over z).
Axes of the slice: x: 2, y: 2, z: 4, core: 2. Of those that a mesh axis runs over, the one named last changes fastest.
Arguments:
- queries: bfloat16 [32, 4096], P(('req', 'kv')), may hold values from -16 to 16
- paged_key_cache: bfloat16 [192, 128, 1024], P(('req', 'kv')), may hold values from -8 to 8
- paged_value_cache: bfloat16 [192, 128, 1024], P(('req', 'kv')), may hold values from -6 to 6
- page_request: int32 [192], P(('req', 'kv')), may hold values from 0 to 31, as said below
- page_number: int32 [192], P(('req', 'kv')), may hold values from 0 to 7, as said below
- lengths: int32 [32], replicated, may hold values from 1 to 1024, as said below
Outputs:
- attended: bfloat16 [32, 4096], P(('req', 'kv'))
The draws below stay inside these ranges and needn't reach their ends.
Inputs may be any that keep to these rules, and one draw needn't show every extreme that they name: `page_request`: every request has 1 to 8 pages and some request exactly 8; the 6 slots of one device hold pages of requests r with 6 different values of r // 4. `page_number`: the pages of one request are numbered 0, 1, 2 and so on without gaps, each number once. `lengths`: a request with n pages has a length from (n - 1) * 128 + 1 to n * 128.
All inputs are finite; a program needn't handle non-finite values.
Results may differ from the reference program's by a relative error of at most 0.0023.
Values may be sent and summed in bfloat16 or wider, within the bound.
A program may use at most 64 MiB of HBM per device.

```python
import jax
import jax.numpy as jnp
from jax import lax

HQ = 32
KEY_VALUE_HEADS = 8
HEAD_SIZE = 128
PAGE_TOKENS = 128
DEVICE_PAGES = 6
QUERY_PER_KV = 4
REQUESTS = 32
TOTAL_PAGES = 192
MOST_PAGES = 8
DEVICES = 32


def page_tables(key):
    base = jax.random.fold_in(key, 11)
    streams = jax.random.split(base, 7)
    relabel = jax.random.permutation(streams[0], REQUESTS).astype(jnp.int32)
    starts = jax.random.randint(streams[1], (REQUESTS,), 0, 1024).astype(jnp.int32)
    slopes = jax.random.randint(streams[2], (REQUESTS,), 1, 65).astype(jnp.int32)
    forced = relabel[0]
    starts = starts.at[forced].set(4096)
    slopes = slopes.at[forced].set(1)
    cells = REQUESTS * MOST_PAGES
    ranks = jnp.arange(MOST_PAGES, dtype=jnp.int32)
    ties = jax.random.permutation(streams[3], cells).astype(jnp.int32).reshape(REQUESTS, MOST_PAGES)
    score = (starts[:, None] - ranks[None, :] * slopes[:, None]) * cells + ties
    score = jnp.where(ranks[None, :] == 0, 2 ** 30, score).reshape(cells)
    order = jnp.argsort(-score)
    chosen = jnp.zeros((cells,), jnp.int32).at[order[:TOTAL_PAGES]].set(1)
    flat = jnp.arange(cells, dtype=jnp.int32)
    listing = jnp.argsort((1 - chosen) * cells + flat)[:TOTAL_PAGES].astype(jnp.int32)
    request_of = listing // MOST_PAGES
    number_of = listing % MOST_PAGES
    places = jnp.arange(TOTAL_PAGES, dtype=jnp.int32)
    shuffle = jax.random.permutation(streams[4], DEVICES).astype(jnp.int32)
    device = jnp.take(shuffle, places % DEVICES)
    offsets = jax.random.randint(streams[5], (DEVICES,), 0, DEVICE_PAGES).astype(jnp.int32)
    slot = (places // DEVICES + jnp.take(offsets, device)) % DEVICE_PAGES
    position = device * DEVICE_PAGES + slot
    owners = jnp.zeros((TOTAL_PAGES,), jnp.int32).at[position].set(request_of)
    numbers = jnp.zeros((TOTAL_PAGES,), jnp.int32).at[position].set(number_of)
    counts = jnp.sum(chosen.reshape(REQUESTS, MOST_PAGES), axis=1)
    extra = jax.random.randint(streams[6], (REQUESTS,), 1, PAGE_TOKENS + 1)
    request_lengths = ((counts - 1) * PAGE_TOKENS + extra).astype(jnp.int32)
    return (owners, numbers, request_lengths)


def draw_page_request(key, part):
    return page_tables(key)[0]


def draw_page_number(key, part):
    return page_tables(key)[1]


def draw_lengths(key, part):
    return page_tables(key)[2]


def draw_queries(key, part):
    random_noise = jax.random.normal(jax.random.fold_in(key, 21), (REQUESTS, HQ, HEAD_SIZE), jnp.float32)
    result = jnp.clip(2.5 * random_noise, -16.0, 16.0)
    return result.reshape(REQUESTS, HQ * HEAD_SIZE).astype(jnp.bfloat16)


def draw_paged_key_cache(key, part):
    random_noise = jnp.clip(jax.random.normal(jax.random.fold_in(key, 41), (TOTAL_PAGES, PAGE_TOKENS, KEY_VALUE_HEADS, HEAD_SIZE), jnp.float32), -6.0, 6.0)
    return random_noise.reshape(TOTAL_PAGES, PAGE_TOKENS, KEY_VALUE_HEADS * HEAD_SIZE).astype(jnp.bfloat16)


def level_of(stream_key, extent, cuts, least, top_value):
    gain = 1.0
    for axis_at, parts in cuts:
        draws = jax.random.uniform(jax.random.fold_in(jax.random.fold_in(stream_key, 6), axis_at), (parts,), jnp.float32, least / len(cuts), top_value / len(cuts))
        gain = gain * jnp.repeat(jnp.exp(draws), extent[axis_at] // parts).reshape((-1,) + (1,) * (len(extent) - 1 - axis_at))
    return gain


def noise(rng, shape, width, most, cuts=(), kind=jnp.bfloat16):
    drawn = width * jax.random.normal(rng, shape, jnp.float32)
    if cuts:
        drawn = drawn * level_of(rng, shape, cuts, -0.22, 0.18)
    return jnp.clip(drawn, -most, most).astype(kind)


def setup_inputs(seed: int = 0) -> dict:
    key_of = jax.random.split(jax.random.key(seed), 7)
    queries = draw_queries(jax.random.fold_in(key_of[6], 71), 0)
    paged_key_cache = draw_paged_key_cache(jax.random.fold_in(key_of[6], 71), 0)
    paged_value_cache = noise(key_of[2], (TOTAL_PAGES, PAGE_TOKENS, KEY_VALUE_HEADS * HEAD_SIZE), 1.0, 6.0, ((0, 32),))
    page_request = draw_page_request(jax.random.fold_in(key_of[6], 71), 0)
    page_number = draw_page_number(jax.random.fold_in(key_of[6], 71), 0)
    lengths = draw_lengths(jax.random.fold_in(key_of[6], 71), 0)
    return dict(queries=queries, paged_key_cache=paged_key_cache, paged_value_cache=paged_value_cache, page_request=page_request, page_number=page_number, lengths=lengths)


lowest = -1e30


def page_attention(gathered_query_rows, gathered_key_rows, gathered_value_rows, usable):
    token_count = gathered_query_rows.shape[0]
    query_single = gathered_query_rows.astype(jnp.float32).reshape(token_count, KEY_VALUE_HEADS, QUERY_PER_KV, HEAD_SIZE)
    key_single = gathered_key_rows.astype(jnp.float32).reshape(token_count, PAGE_TOKENS, KEY_VALUE_HEADS, HEAD_SIZE)
    value_single = gathered_value_rows.astype(jnp.float32).reshape(token_count, PAGE_TOKENS, KEY_VALUE_HEADS, HEAD_SIZE)
    scores = jnp.einsum("sgqd,stgd->sgqt", query_single, key_single, precision=lax.Precision.HIGHEST) * (HEAD_SIZE ** -0.5)
    scores = jnp.where(usable[:, None, None, :], scores, lowest)
    maxima = jnp.max(scores, axis=-1)
    weights = jnp.exp(scores - maxima[..., None])
    sums_exp = jnp.sum(weights, axis=-1)
    rounded = weights.astype(jnp.bfloat16).astype(jnp.float32)
    partial_out = jnp.einsum("sgqt,stgd->sgqd", rounded, value_single, precision=lax.Precision.HIGHEST)
    return maxima.reshape(token_count, HQ), sums_exp.reshape(token_count, HQ), partial_out.reshape(token_count, HQ * HEAD_SIZE)


def reference(queries, paged_key_cache, paged_value_cache, page_request, page_number, lengths):
    request_blocks = page_request.reshape(DEVICES, DEVICE_PAGES)
    number_blocks = page_number.reshape(DEVICES, DEVICE_PAGES)
    paged_key_blocks = paged_key_cache.reshape(DEVICES, DEVICE_PAGES, PAGE_TOKENS, KEY_VALUE_HEADS * HEAD_SIZE)
    paged_value_blocks = paged_value_cache.reshape(DEVICES, DEVICE_PAGES, PAGE_TOKENS, KEY_VALUE_HEADS * HEAD_SIZE)
    positions = jnp.arange(PAGE_TOKENS, dtype=jnp.int32)

    def per_block(block):
        owners, numbers, gathered_key_rows, gathered_value_rows = block
        gathered_query_rows = jnp.take(queries, owners, axis=0)
        limits = jnp.take(lengths, owners)
        usable = numbers[:, None] * PAGE_TOKENS + positions[None, :] < limits[:, None]
        return page_attention(gathered_query_rows, gathered_key_rows, gathered_value_rows, usable)

    maxima, sums_exp, partial_out = lax.map(per_block, (request_blocks, number_blocks, paged_key_blocks, paged_value_blocks))
    maxima = maxima.reshape(TOTAL_PAGES, HQ)
    sums_exp = sums_exp.reshape(TOTAL_PAGES, HQ)
    partial_out = partial_out.reshape(TOTAL_PAGES, HQ, HEAD_SIZE)
    request_max = jnp.full((REQUESTS, HQ), lowest, jnp.float32).at[page_request].max(maxima)
    factors = jnp.exp(maxima - jnp.take(request_max, page_request, axis=0))
    numerators = jnp.zeros((REQUESTS, HQ, HEAD_SIZE), jnp.float32).at[page_request].add(factors[:, :, None] * partial_out)
    denominators = jnp.zeros((REQUESTS, HQ), jnp.float32).at[page_request].add(factors * sums_exp)
    attended = numerators / denominators[:, :, None]
    return attended.reshape(REQUESTS, HQ * HEAD_SIZE).astype(jnp.bfloat16)
```

```python
import functools

import jax
import jax.numpy as jnp
from jax import lax
from jax.experimental import pallas as pl
from jax.experimental.pallas import tpu as pltpu
from jax.sharding import PartitionSpec as P

HQ = 32
KEY_VALUE_HEADS = 8
HEAD_SIZE = 128
QUERY_PER_KV = 4
PAIR = 2 * QUERY_PER_KV
STAT = 8

lowest = -1e30
MESH = pl.DeviceIdType.MESH


def diagonal_to_lanes(column, on_diagonal):
    return jnp.sum(jnp.where(on_diagonal, column, 0.0), axis=0, keepdims=True)


def lanes_to_column(row, on_diagonal):
    return jnp.sum(jnp.where(on_diagonal, row, 0.0), axis=1, keepdims=True)


def kernel(
    n_req, n_kv, group,
    owner_ref, number_ref, length_ref, q_ref, key_hbm, value_hbm, out_ref,
    keys, values, q_rows, q_group, table, q_send, q_in, parts, part_send, part_in, merged, merged_in,
    page_sem, qs_sem, qr_sem, ts_sem, tr_sem, ds_sem, dr_sem, ps_sem, pr_sem, ms_sem, mr_sem,
):
    slots, page_tokens, _ = keys.shape
    my_req = lax.axis_index("req")
    my_kv = lax.axis_index("kv")

    loads = []
    for s in range(slots):
        loads.append(pltpu.make_async_copy(key_hbm.at[s], keys.at[s], page_sem.at[0, s]))
        loads.append(pltpu.make_async_copy(value_hbm.at[s], values.at[s], page_sem.at[1, s]))
    for load in loads:
        load.start()

    barrier = pltpu.get_barrier_semaphore()
    req_peers = [lax.rem(my_req + d, n_req) for d in range(n_req)]
    kv_peers = [lax.rem(my_kv + d, n_kv) for d in range(n_kv)]
    for d in range(1, n_req):
        pl.semaphore_signal(barrier, inc=1, device_id=(req_peers[d], my_kv), device_id_type=MESH)
    for d in range(1, n_kv):
        pl.semaphore_signal(barrier, inc=1, device_id=(my_req, kv_peers[d]), device_id_type=MESH)

    for h in range(HQ):
        q_rows[h : h + 1, :] = q_ref[0:1, h * HEAD_SIZE : (h + 1) * HEAD_SIZE].astype(jnp.float32)
    q_group[my_kv] = q_rows[...].astype(jnp.bfloat16)
    lane8 = lax.broadcasted_iota(jnp.int32, (STAT, HEAD_SIZE), 1)
    sub8 = lax.broadcasted_iota(jnp.int32, (STAT, HEAD_SIZE), 0)
    own_table = jnp.full((STAT, HEAD_SIZE), -1.0, jnp.float32)
    for s in range(slots):
        own_table = jnp.where(lane8 == s, owner_ref[s].astype(jnp.float32), own_table)
    table[my_req] = own_table

    pl.semaphore_wait(barrier, n_req - 1 + n_kv - 1)

    def remote(src, dst, send, recv, target):
        return pltpu.make_async_remote_copy(
            src_ref=src, dst_ref=dst, send_sem=send, recv_sem=recv,
            device_id=target, device_id_type=MESH,
        )

    sent = []
    table_copies, query_copies = [None], [None]
    for d in range(1, n_kv):
        copy = remote(q_group.at[my_kv], q_group.at[my_kv], qs_sem.at[d], qr_sem.at[d], (my_req, kv_peers[d]))
        copy.start()
        query_copies.append(copy)
    for d in range(1, n_req):
        copy = remote(table.at[my_req], table.at[my_req], ts_sem.at[d], tr_sem.at[d], (req_peers[d], my_kv))
        copy.start()
        table_copies.append(copy)

    for copy in table_copies[1:]:
        copy.wait()
    base = (my_req * group).astype(jnp.float32)
    held = []
    for d in range(n_req):
        rel = table[req_peers[d]] - base
        inside = jnp.logical_and(rel >= 0.0, rel < float(group))
        held.append(jnp.max(jnp.where(inside, rel, -1.0), axis=1, keepdims=True)[0:1])
    for copy in query_copies[1:]:
        copy.wait()

    choices = [q_group[c].astype(jnp.float32) for c in range(group)]
    for d in list(range(1, n_req)) + [0]:
        pick = jnp.broadcast_to(held[d], (HQ, HEAD_SIZE))
        chosen = jnp.zeros((HQ, HEAD_SIZE), jnp.float32)
        for c in range(group):
            chosen = jnp.where(pick == float(c), choices[c], chosen)
        if d == 0:
            q_in[my_req] = chosen.astype(jnp.bfloat16)
            continue
        q_send[d] = chosen.astype(jnp.bfloat16)
        copy = remote(q_send.at[d], q_in.at[my_req], ds_sem.at[d], dr_sem.at[d], (req_peers[d], my_kv))
        copy.start()
        sent.append(copy)

    for load in loads:
        load.wait()
    for copy in sent:
        copy.wait()

    row = lax.broadcasted_iota(jnp.int32, (HQ, HEAD_SIZE), 0)
    lane = lax.broadcasted_iota(jnp.int32, (HQ, HEAD_SIZE), 1)
    on_diagonal = row == lane
    first = sub8 < QUERY_PER_KV
    token = lax.broadcasted_iota(jnp.int32, (HQ, page_tokens), 1)
    wide = 2 * HEAD_SIZE

    parts[slots, 0:HQ, :] = jnp.zeros((HQ, HEAD_SIZE), jnp.float32)
    parts[slots, HQ : HQ + STAT, :] = jnp.where(sub8 == 0, lowest, 0.0)
    for s in range(slots):
        request = owner_ref[s]
        query = q_in[lax.div(request, group)].astype(jnp.float32)
        limit = length_ref[request] - number_ref[s] * page_tokens
        pieces = []
        for k in range(HQ // PAIR):
            q8 = query[k * PAIR : (k + 1) * PAIR]
            both = jnp.concatenate(
                [jnp.where(first, q8, 0.0), jnp.where(first, 0.0, q8)], axis=1
            ).astype(jnp.bfloat16)
            pieces.append(
                lax.dot_general(
                    both, keys[s, :, k * wide : (k + 1) * wide],
                    (((1,), (1,)), ((), ())), preferred_element_type=jnp.float32,
                )
            )
        scores = jnp.concatenate(pieces, axis=0) * HEAD_SIZE ** (-0.5)
        scores = jnp.where(token < limit, scores, lowest)
        top = jnp.max(scores, axis=1, keepdims=True)
        weights = jnp.exp(scores - top)
        total = jnp.sum(weights, axis=1, keepdims=True)
        for k in range(HQ // PAIR):
            w8 = weights[k * PAIR : (k + 1) * PAIR].astype(jnp.bfloat16)
            both = jnp.dot(
                w8, values[s, :, k * wide : (k + 1) * wide], preferred_element_type=jnp.float32
            )
            parts[s, k * PAIR : (k + 1) * PAIR, :] = jnp.where(
                first, both[:, :HEAD_SIZE], both[:, HEAD_SIZE:]
            )
        parts[s, HQ : HQ + STAT, :] = jnp.where(
            sub8 == 0, diagonal_to_lanes(top, on_diagonal), diagonal_to_lanes(total, on_diagonal)
        )

    sent = []
    for d in list(range(1, n_req)) + [0]:
        index = jnp.int32(slots)
        for s in range(slots):
            index = jnp.where(lax.div(owner_ref[s], group) == req_peers[d], jnp.int32(s), index)
        block = parts[index]
        if d == 0:
            part_in[my_req] = block
            continue
        part_send[d] = block
        copy = remote(part_send.at[d], part_in.at[my_req], ps_sem.at[d], pr_sem.at[d], (req_peers[d], my_kv))
        copy.start()
        sent.append(copy)
    for copy in sent:
        copy.wait()

    tops, totals = [], []
    for d in range(n_req):
        tops.append(part_in[req_peers[d], HQ : HQ + 1, :])
        totals.append(part_in[req_peers[d], HQ + 1 : HQ + 2, :])
    merged_top, merged_total = [], []
    factors = [jnp.zeros((1, HEAD_SIZE), jnp.float32) for _ in range(n_req)]
    member = [[jnp.broadcast_to(held[d], (1, HEAD_SIZE)) == float(c) for d in range(n_req)] for c in range(group)]
    for c in range(group):
        best = jnp.full((1, HEAD_SIZE), lowest, jnp.float32)
        for d in range(n_req):
            best = jnp.maximum(best, jnp.where(member[c][d], tops[d], lowest))
        merged_top.append(best)
    for d in range(n_req):
        best = tops[d]
        for c in range(group):
            best = jnp.where(member[c][d], merged_top[c], best)
        factors[d] = jnp.exp(tops[d] - best)
    for c in range(group):
        amount = jnp.zeros((1, HEAD_SIZE), jnp.float32)
        for d in range(n_req):
            amount = amount + jnp.where(member[c][d], factors[d] * totals[d], 0.0)
        merged_total.append(amount)
    sums = [jnp.zeros((HQ, HEAD_SIZE), jnp.float32) for _ in range(group)]
    for d in range(n_req):
        scaled = lanes_to_column(factors[d], on_diagonal) * part_in[req_peers[d], 0:HQ, :]
        pick = jnp.broadcast_to(held[d], (HQ, HEAD_SIZE))
        for c in range(group):
            sums[c] = sums[c] + jnp.where(pick == float(c), scaled, 0.0)
    for c in range(group):
        merged[c, 0:HQ, :] = sums[c]
        merged[c, HQ : HQ + STAT, :] = jnp.where(sub8 == 0, merged_top[c], merged_total[c])

    sent = []
    for d in range(1, n_kv):
        copy = remote(merged.at[kv_peers[d]], merged_in.at[my_kv], ms_sem.at[d], mr_sem.at[d], (my_req, kv_peers[d]))
        copy.start()
        sent.append(copy)
    merged_in[my_kv] = merged[my_kv]
    for copy in sent:
        copy.wait()

    tops = [merged_in[c, HQ : HQ + 1, :] for c in range(n_kv)]
    best = tops[0]
    for c in range(1, n_kv):
        best = jnp.maximum(best, tops[c])
    factors = [jnp.exp(tops[c] - best) for c in range(n_kv)]
    amount = jnp.zeros((1, HEAD_SIZE), jnp.float32)
    for c in range(n_kv):
        amount = amount + factors[c] * merged_in[c, HQ + 1 : HQ + 2, :]
    result = jnp.zeros((HQ, HEAD_SIZE), jnp.float32)
    for c in range(n_kv):
        result = result + lanes_to_column(factors[c], on_diagonal) * merged_in[c, 0:HQ, :]
    result = result / lanes_to_column(amount, on_diagonal)
    out_ref[...] = result.astype(jnp.bfloat16)


def solution(mesh):
    n_req, n_kv = mesh.shape["req"], mesh.shape["kv"]

    def on_device(queries, key_cache, value_cache, page_request, page_number, lengths):
        slots, page_tokens, width = key_cache.shape
        group = lengths.shape[0] // n_req
        dma = pltpu.SemaphoreType.DMA
        smem = pl.BlockSpec(memory_space=pltpu.SMEM)
        vmem = pl.BlockSpec(memory_space=pltpu.VMEM)
        anywhere = pl.BlockSpec(memory_space=pl.ANY)
        blob = (HQ + STAT, HEAD_SIZE)
        attended = pl.pallas_call(
            functools.partial(kernel, n_req, n_kv, group),
            out_shape=jax.ShapeDtypeStruct((HQ, HEAD_SIZE), jnp.bfloat16),
            in_specs=[smem, smem, smem, vmem, anywhere, anywhere],
            out_specs=vmem,
            scratch_shapes=[
                pltpu.VMEM((slots, page_tokens, width), jnp.bfloat16),
                pltpu.VMEM((slots, page_tokens, width), jnp.bfloat16),
                pltpu.VMEM((HQ, HEAD_SIZE), jnp.float32),
                pltpu.VMEM((n_kv, HQ, HEAD_SIZE), jnp.bfloat16),
                pltpu.VMEM((n_req, STAT, HEAD_SIZE), jnp.float32),
                pltpu.VMEM((n_req, HQ, HEAD_SIZE), jnp.bfloat16),
                pltpu.VMEM((n_req, HQ, HEAD_SIZE), jnp.bfloat16),
                pltpu.VMEM((slots + 1,) + blob, jnp.float32),
                pltpu.VMEM((n_req,) + blob, jnp.float32),
                pltpu.VMEM((n_req,) + blob, jnp.float32),
                pltpu.VMEM((group,) + blob, jnp.float32),
                pltpu.VMEM((n_kv,) + blob, jnp.float32),
                dma((2, slots)),
                dma((n_kv,)), dma((n_kv,)),
                dma((n_req,)), dma((n_req,)),
                dma((n_req,)), dma((n_req,)),
                dma((n_req,)), dma((n_req,)),
                dma((n_kv,)), dma((n_kv,)),
            ],
            compiler_params=pltpu.CompilerParams(collective_id=0, has_side_effects=True),
        )(page_request, page_number, lengths, queries, key_cache, value_cache)
        return attended.reshape(queries.shape)

    placed = (
        P(("req", "kv"), None),
        P(("req", "kv"), None, None),
        P(("req", "kv"), None, None),
        P(("req", "kv")),
        P(("req", "kv")),
        P(),
    )
    return jax.shard_map(
        on_device, mesh=mesh, in_specs=placed, out_specs=P(("req", "kv"), None), check_vma=False
    )
```

```python
import functools

import jax
import jax.numpy as jnp
from jax import lax
from jax.experimental import pallas as pl
from jax.experimental.pallas import tpu as pltpu
from jax.sharding import PartitionSpec as P

HQ = 32
KEY_VALUE_HEADS = 8
HEAD_SIZE = 128
QUERY_PER_KV = 4
PAIR = 2 * QUERY_PER_KV
STAT = 8

lowest = -1e30
MESH = pl.DeviceIdType.MESH


def partners(me, n):
    if n & (n - 1):
        return [lax.rem(me + d, n) for d in range(n)]
    found = []
    for d in range(n):
        place, bit = me, 1
        while bit < n:
            if d & bit:
                place = place + bit - 2 * bit * lax.rem(lax.div(me, bit), 2)
            bit *= 2
        found.append(place)
    return found


def diagonal_to_lanes(column, on_diagonal):
    return jnp.sum(jnp.where(on_diagonal, column, 0.0), axis=0, keepdims=True)


def lanes_to_column(row, on_diagonal):
    return jnp.sum(jnp.where(on_diagonal, row, 0.0), axis=1, keepdims=True)


def kernel(
    n_req, n_kv, group,
    owner_hbm, number_hbm, length_hbm, q_hbm, key_hbm, value_hbm, out_ref,
    owner_ref, number_ref, length_ref, q_ref, keys, values, q_rows, q_group, table, q_send, q_in, part_send, part_in, merged, merged_in,
    small_sem, page_sem, qs_sem, qr_sem, ts_sem, tr_sem, ds_sem, dr_sem, ps_sem, pr_sem, ms_sem, mr_sem,
):
    slots, page_tokens, _ = keys.shape
    my_req = lax.axis_index("req")
    my_kv = lax.axis_index("kv")

    small = [
        pltpu.make_async_copy(src, dst, small_sem.at[i])
        for i, (src, dst) in enumerate(
            ((q_hbm, q_ref), (owner_hbm, owner_ref), (number_hbm, number_ref), (length_hbm, length_ref))
        )
    ]
    for copy in small:
        copy.start()

    loads = []
    for s in range(slots):
        loads.append(pltpu.make_async_copy(key_hbm.at[s], keys.at[s], page_sem.at[0, s]))
        loads.append(pltpu.make_async_copy(value_hbm.at[s], values.at[s], page_sem.at[1, s]))
    barrier = pltpu.get_barrier_semaphore()
    req_peers = partners(my_req, n_req)
    kv_peers = partners(my_kv, n_kv)
    for d in range(1, n_req):
        pl.semaphore_signal(barrier, inc=1, device_id=(req_peers[d], my_kv), device_id_type=MESH)
    for d in range(1, n_kv):
        pl.semaphore_signal(barrier, inc=1, device_id=(my_req, kv_peers[d]), device_id_type=MESH)

    for load in loads:
        load.start()
    for copy in small:
        copy.wait()

    for h in range(HQ):
        q_rows[h : h + 1, :] = q_ref[0:1, h * HEAD_SIZE : (h + 1) * HEAD_SIZE].astype(jnp.float32)
    q_group[my_kv] = q_rows[...].astype(jnp.bfloat16)
    lane8 = lax.broadcasted_iota(jnp.int32, (STAT, HEAD_SIZE), 1)
    sub8 = lax.broadcasted_iota(jnp.int32, (STAT, HEAD_SIZE), 0)
    own_table = jnp.full((STAT, HEAD_SIZE), -1.0, jnp.float32)
    for s in range(slots):
        own_table = jnp.where(lane8 == s, owner_ref[s].astype(jnp.float32), own_table)
    table[my_req] = own_table

    pl.semaphore_wait(barrier, n_req - 1 + n_kv - 1)

    def remote(src, dst, send, recv, target):
        return pltpu.make_async_remote_copy(
            src_ref=src, dst_ref=dst, send_sem=send, recv_sem=recv,
            device_id=target, device_id_type=MESH,
        )

    sent = []
    table_copies, query_copies = [None], [None]
    for d in range(n_kv - 1, 0, -1):
        copy = remote(q_group.at[my_kv], q_group.at[my_kv], qs_sem.at[d], qr_sem.at[d], (my_req, kv_peers[d]))
        copy.start()
        query_copies.append(copy)
    for d in range(n_req - 1, 0, -1):
        copy = remote(table.at[my_req], table.at[my_req], ts_sem.at[d], tr_sem.at[d], (req_peers[d], my_kv))
        copy.start()
        table_copies.append(copy)

    homes = []
    for d in range(n_req):
        index, present = jnp.int32(0), jnp.int32(0)
        for s in range(slots):
            same = lax.div(owner_ref[s], group) == req_peers[d]
            index = jnp.where(same, jnp.int32(s), index)
            present = jnp.where(same, jnp.int32(1), present)
        limit = length_ref[owner_ref[index]] - number_ref[index] * page_tokens
        homes.append((index, limit * present))

    for copy in table_copies[1:]:
        copy.wait()
    base = (my_req * group).astype(jnp.float32)
    held = []
    for d in range(n_req):
        rel = table[req_peers[d]] - base
        inside = jnp.logical_and(rel >= 0.0, rel < float(group))
        held.append(jnp.max(jnp.where(inside, rel, -1.0), axis=1, keepdims=True)[0:1])
    for copy in query_copies[1:]:
        copy.wait()

    choices = [q_group[c].astype(jnp.float32) for c in range(group)]
    query_in = [None] * n_req
    for d in list(range(n_req - 1, -1, -1)):
        pick = jnp.broadcast_to(held[d], (HQ, HEAD_SIZE))
        chosen = jnp.zeros((HQ, HEAD_SIZE), jnp.float32)
        for c in range(group):
            chosen = jnp.where(pick == float(c), choices[c], chosen)
        if d == 0:
            q_in[my_req] = chosen.astype(jnp.bfloat16)
            continue
        q_send[d] = chosen.astype(jnp.bfloat16)
        copy = remote(q_send.at[d], q_in.at[my_req], ds_sem.at[d], dr_sem.at[d], (req_peers[d], my_kv))
        copy.start()
        query_in[d] = copy

    for load in loads:
        load.wait()

    row = lax.broadcasted_iota(jnp.int32, (HQ, HEAD_SIZE), 0)
    lane = lax.broadcasted_iota(jnp.int32, (HQ, HEAD_SIZE), 1)
    on_diagonal = row == lane
    first = sub8 < QUERY_PER_KV
    token = lax.broadcasted_iota(jnp.int32, (HQ, page_tokens), 1)
    wide = 2 * HEAD_SIZE

    part_copies = [None] * n_req
    edges = [0, max(n_req // 4, 1), max(3 * n_req // 4, 1), n_req]
    for low, high in zip(edges[:-1], edges[1:]):
        batch = range(high - 1, low - 1, -1)
        for d in batch:
            if d:
                query_in[d].wait()
        scored = {}
        for d in batch:
            index, limit = homes[d]
            query = q_in[req_peers[d]].astype(jnp.float32)
            pieces = []
            for k in range(HQ // PAIR):
                q8 = query[k * PAIR : (k + 1) * PAIR]
                both = jnp.concatenate(
                    [jnp.where(first, q8, 0.0), jnp.where(first, 0.0, q8)], axis=1
                ).astype(jnp.bfloat16)
                pieces.append(
                    lax.dot_general(
                        both, keys[index, :, k * wide : (k + 1) * wide],
                        (((1,), (1,)), ((), ())), preferred_element_type=jnp.float32,
                    )
                )
            scores = jnp.concatenate(pieces, axis=0) * HEAD_SIZE ** (-0.5)
            scored[d] = jnp.where(token < limit, scores, lowest)
        tops = {d: jnp.max(scored[d], axis=1, keepdims=True) for d in batch}
        weights = {d: jnp.exp(scored[d] - tops[d]) for d in batch}
        totals = {d: jnp.sum(weights[d], axis=1, keepdims=True) for d in batch}
        for d in batch:
            index, limit = homes[d]
            blocks = []
            for k in range(HQ // PAIR):
                w8 = weights[d][k * PAIR : (k + 1) * PAIR].astype(jnp.bfloat16)
                both = jnp.dot(
                    w8, values[index, :, k * wide : (k + 1) * wide], preferred_element_type=jnp.float32
                )
                blocks.append(jnp.where(first, both[:, :HEAD_SIZE], both[:, HEAD_SIZE:]))
            blocks.append(
                jnp.where(
                    sub8 == 0,
                    diagonal_to_lanes(tops[d], on_diagonal),
                    diagonal_to_lanes(totals[d], on_diagonal),
                )
            )
            block = jnp.concatenate(blocks, axis=0)
            if d == 0:
                part_in[my_req] = block
                continue
            part_send[d] = block
            copy = remote(part_send.at[d], part_in.at[my_req], ps_sem.at[d], pr_sem.at[d], (req_peers[d], my_kv))
            copy.start()
            part_copies[d] = copy
    for copy in part_copies[1:]:
        copy.wait()

    tops, totals = [], []
    for d in range(n_req):
        tops.append(part_in[req_peers[d], HQ : HQ + 1, :])
        totals.append(part_in[req_peers[d], HQ + 1 : HQ + 2, :])
    merged_top, merged_total = [], []
    factors = [jnp.zeros((1, HEAD_SIZE), jnp.float32) for _ in range(n_req)]
    member = [[jnp.broadcast_to(held[d], (1, HEAD_SIZE)) == float(c) for d in range(n_req)] for c in range(group)]
    for c in range(group):
        best = jnp.full((1, HEAD_SIZE), lowest, jnp.float32)
        for d in range(n_req):
            best = jnp.maximum(best, jnp.where(member[c][d], tops[d], lowest))
        merged_top.append(best)
    for d in range(n_req):
        best = tops[d]
        for c in range(group):
            best = jnp.where(member[c][d], merged_top[c], best)
        factors[d] = jnp.exp(tops[d] - best)
    for c in range(group):
        amount = jnp.zeros((1, HEAD_SIZE), jnp.float32)
        for d in range(n_req):
            amount = amount + jnp.where(member[c][d], factors[d] * totals[d], 0.0)
        merged_total.append(amount)
    sums = [jnp.zeros((HQ, HEAD_SIZE), jnp.float32) for _ in range(group)]
    for d in range(n_req):
        scaled = lanes_to_column(factors[d], on_diagonal) * part_in[req_peers[d], 0:HQ, :]
        pick = jnp.broadcast_to(held[d], (HQ, HEAD_SIZE))
        for c in range(group):
            sums[c] = sums[c] + jnp.where(pick == float(c), scaled, 0.0)
    for c in range(group):
        merged[c, 0:HQ, :] = sums[c]
        merged[c, HQ : HQ + STAT, :] = jnp.where(sub8 == 0, merged_top[c], merged_total[c])

    sent = []
    for d in range(n_kv - 1, 0, -1):
        copy = remote(merged.at[kv_peers[d]], merged_in.at[my_kv], ms_sem.at[d], mr_sem.at[d], (my_req, kv_peers[d]))
        copy.start()
        sent.append(copy)
    merged_in[my_kv] = merged[my_kv]
    for copy in sent:
        copy.wait()

    tops = [merged_in[c, HQ : HQ + 1, :] for c in range(n_kv)]
    best = tops[0]
    for c in range(1, n_kv):
        best = jnp.maximum(best, tops[c])
    factors = [jnp.exp(tops[c] - best) for c in range(n_kv)]
    amount = jnp.zeros((1, HEAD_SIZE), jnp.float32)
    for c in range(n_kv):
        amount = amount + factors[c] * merged_in[c, HQ + 1 : HQ + 2, :]
    result = jnp.zeros((HQ, HEAD_SIZE), jnp.float32)
    for c in range(n_kv):
        result = result + lanes_to_column(factors[c], on_diagonal) * merged_in[c, 0:HQ, :]
    result = result / lanes_to_column(amount, on_diagonal)
    out_ref[...] = result.astype(jnp.bfloat16)


def solution(mesh):
    n_req, n_kv = mesh.shape["req"], mesh.shape["kv"]

    def on_device(queries, key_cache, value_cache, page_request, page_number, lengths):
        slots, page_tokens, width = key_cache.shape
        group = lengths.shape[0] // n_req
        dma = pltpu.SemaphoreType.DMA
        vmem = pl.BlockSpec(memory_space=pltpu.VMEM)
        anywhere = pl.BlockSpec(memory_space=pl.ANY)
        blob = (HQ + STAT, HEAD_SIZE)
        attended = pl.pallas_call(
            functools.partial(kernel, n_req, n_kv, group),
            out_shape=pltpu.VMEM((HQ, HEAD_SIZE), jnp.bfloat16),
            in_specs=[anywhere] * 6,
            out_specs=vmem,
            scratch_shapes=[
                pltpu.SMEM(page_request.shape, jnp.int32),
                pltpu.SMEM(page_number.shape, jnp.int32),
                pltpu.SMEM(lengths.shape, jnp.int32),
                pltpu.VMEM(queries.shape, queries.dtype),
                pltpu.VMEM((slots, page_tokens, width), jnp.bfloat16),
                pltpu.VMEM((slots, page_tokens, width), jnp.bfloat16),
                pltpu.VMEM((HQ, HEAD_SIZE), jnp.float32),
                pltpu.VMEM((n_kv, HQ, HEAD_SIZE), jnp.bfloat16),
                pltpu.VMEM((n_req, STAT, HEAD_SIZE), jnp.float32),
                pltpu.VMEM((n_req, HQ, HEAD_SIZE), jnp.bfloat16),
                pltpu.VMEM((n_req, HQ, HEAD_SIZE), jnp.bfloat16),
                pltpu.VMEM((n_req,) + blob, jnp.float32),
                pltpu.VMEM((n_req,) + blob, jnp.float32),
                pltpu.VMEM((group,) + blob, jnp.float32),
                pltpu.VMEM((n_kv,) + blob, jnp.float32),
                dma((4,)),
                dma((2, slots)),
                dma((n_kv,)), dma((n_kv,)),
                dma((n_req,)), dma((n_req,)),
                dma((n_req,)), dma((n_req,)),
                dma((n_req,)), dma((n_req,)),
                dma((n_kv,)), dma((n_kv,)),
            ],
            compiler_params=pltpu.CompilerParams(collective_id=0, has_side_effects=True),
        )(page_request, page_number, lengths, queries, key_cache, value_cache)
        return attended.reshape(queries.shape)

    placed = (
        P(("req", "kv"), None),
        P(("req", "kv"), None, None),
        P(("req", "kv"), None, None),
        P(("req", "kv")),
        P(("req", "kv")),
        P(),
    )
    return jax.shard_map(
        on_device, mesh=mesh, in_specs=placed, out_specs=P(("req", "kv"), None), check_vma=False
    )
```

```python
import functools

import jax
import jax.numpy as jnp
from jax import lax
from jax.experimental import pallas as pl
from jax.experimental.pallas import tpu as pltpu
from jax.sharding import PartitionSpec as P

HQ = 32
KEY_VALUE_HEADS = 8
HEAD_SIZE = 128
QUERY_PER_KV = 4
PAIR = 2 * QUERY_PER_KV
STAT = 8

lowest = -1e30
MESH = pl.DeviceIdType.MESH


def partners(me, n):
    if n & (n - 1):
        return [lax.rem(me + d, n) for d in range(n)]
    found = []
    for d in range(n):
        place, bit = me, 1
        while bit < n:
            if d & bit:
                place = place + bit - 2 * bit * lax.rem(lax.div(me, bit), 2)
            bit *= 2
        found.append(place)
    return found


def diagonal_to_lanes(column, on_diagonal):
    return jnp.sum(jnp.where(on_diagonal, column, 0.0), axis=0, keepdims=True)


def lanes_to_column(row, on_diagonal):
    return jnp.sum(jnp.where(on_diagonal, row, 0.0), axis=1, keepdims=True)


def kernel(
    n_req, n_kv, group,
    owner_hbm, number_hbm, length_hbm, q_hbm, key_hbm, value_hbm, out_ref,
    owner_ref, number_ref, length_ref, q_ref, keys, values, q_rows, q_group, table, q_send, q_in, part_send, part_in, merged, merged_in,
    small_sem, page_sem, qs_sem, qr_sem, ts_sem, tr_sem, ds_sem, dr_sem, ps_sem, pr_sem, ms_sem, mr_sem,
):
    slots, page_tokens, _ = keys.shape
    my_req = lax.axis_index("req")
    my_kv = lax.axis_index("kv")

    small = [
        pltpu.make_async_copy(src, dst, small_sem.at[i])
        for i, (src, dst) in enumerate(
            ((q_hbm, q_ref), (owner_hbm, owner_ref), (number_hbm, number_ref), (length_hbm, length_ref))
        )
    ]
    for copy in small:
        copy.start()

    loads = []
    for s in range(slots):
        loads.append(pltpu.make_async_copy(key_hbm.at[s], keys.at[s], page_sem.at[0]))
        loads.append(pltpu.make_async_copy(value_hbm.at[s], values.at[s], page_sem.at[1]))
    barrier = pltpu.get_barrier_semaphore()
    req_peers = partners(my_req, n_req)
    kv_peers = partners(my_kv, n_kv)
    for d in range(1, n_req):
        pl.semaphore_signal(barrier, inc=1, device_id=(req_peers[d], my_kv), device_id_type=MESH)
    for d in range(1, n_kv):
        pl.semaphore_signal(barrier, inc=1, device_id=(my_req, kv_peers[d]), device_id_type=MESH)

    for load in loads:
        load.start()
    for copy in small:
        copy.wait()

    for h in range(HQ):
        q_rows[h : h + 1, :] = q_ref[0:1, h * HEAD_SIZE : (h + 1) * HEAD_SIZE].astype(jnp.float32)
    q_group[my_kv] = q_rows[...].astype(jnp.bfloat16)
    lane8 = lax.broadcasted_iota(jnp.int32, (STAT, HEAD_SIZE), 1)
    sub8 = lax.broadcasted_iota(jnp.int32, (STAT, HEAD_SIZE), 0)
    own_table = jnp.full((STAT, HEAD_SIZE), -1.0, jnp.float32)
    for s in range(slots):
        own_table = jnp.where(lane8 == s, owner_ref[s].astype(jnp.float32), own_table)
    table[my_req] = own_table

    pl.semaphore_wait(barrier, n_req - 1 + n_kv - 1)

    def remote(src, dst, send, recv, target):
        return pltpu.make_async_remote_copy(
            src_ref=src, dst_ref=dst, send_sem=send, recv_sem=recv,
            device_id=target, device_id_type=MESH,
        )

    def arrived(buffer, count, sem):
        if count:
            pltpu.make_async_copy(buffer.at[pl.ds(0, count)], buffer.at[pl.ds(0, count)], sem).wait()

    for d in range(n_kv - 1, 0, -1):
        copy = remote(q_group.at[my_kv], q_group.at[my_kv], qs_sem.at[0], qr_sem.at[0], (my_req, kv_peers[d]))
        copy.start()
    for d in range(n_req - 1, 0, -1):
        copy = remote(table.at[my_req], table.at[my_req], ts_sem.at[0], tr_sem.at[0], (req_peers[d], my_kv))
        copy.start()

    homes = []
    for d in range(n_req):
        index, present = jnp.int32(0), jnp.int32(0)
        for s in range(slots):
            same = lax.div(owner_ref[s], group) == req_peers[d]
            index = jnp.where(same, jnp.int32(s), index)
            present = jnp.where(same, jnp.int32(1), present)
        limit = length_ref[owner_ref[index]] - number_ref[index] * page_tokens
        homes.append((index, limit * present))

    arrived(table, n_req - 1, tr_sem.at[0])
    base = (my_req * group).astype(jnp.float32)
    held = []
    for d in range(n_req):
        rel = table[req_peers[d]] - base
        inside = jnp.logical_and(rel >= 0.0, rel < float(group))
        held.append(jnp.max(jnp.where(inside, rel, -1.0), axis=1, keepdims=True)[0:1])
    arrived(q_group, n_kv - 1, qr_sem.at[0])

    choices = [q_group[c].astype(jnp.float32) for c in range(group)]
    edges = [0, max(n_req // 4, 1), max(3 * n_req // 4, 1), n_req]
    stage_of = [sum(d >= edge for edge in edges[1:]) for d in range(n_req)]
    for d in list(range(n_req - 1, -1, -1)):
        pick = jnp.broadcast_to(held[d], (HQ, HEAD_SIZE))
        chosen = jnp.zeros((HQ, HEAD_SIZE), jnp.float32)
        for c in range(group):
            chosen = jnp.where(pick == float(c), choices[c], chosen)
        if d == 0:
            q_in[my_req] = chosen.astype(jnp.bfloat16)
            continue
        q_send[d] = chosen.astype(jnp.bfloat16)
        copy = remote(q_send.at[d], q_in.at[my_req], ds_sem.at[0], dr_sem.at[stage_of[d]], (req_peers[d], my_kv))
        copy.start()

    pltpu.make_async_copy(key_hbm, keys, page_sem.at[0]).wait()
    pltpu.make_async_copy(value_hbm, values, page_sem.at[1]).wait()

    row = lax.broadcasted_iota(jnp.int32, (HQ, HEAD_SIZE), 0)
    lane = lax.broadcasted_iota(jnp.int32, (HQ, HEAD_SIZE), 1)
    on_diagonal = row == lane
    first = sub8 < QUERY_PER_KV
    token = lax.broadcasted_iota(jnp.int32, (HQ, page_tokens), 1)
    wide = 2 * HEAD_SIZE

    for stage, (low, high) in enumerate(zip(edges[:-1], edges[1:])):
        batch = range(high - 1, low - 1, -1)
        arrived(q_in, high - max(low, 1), dr_sem.at[stage])
        scored = {}
        for d in batch:
            index, limit = homes[d]
            query = q_in[req_peers[d]].astype(jnp.float32)
            pieces = []
            for k in range(HQ // PAIR):
                q8 = query[k * PAIR : (k + 1) * PAIR]
                both = jnp.concatenate(
                    [jnp.where(first, q8, 0.0), jnp.where(first, 0.0, q8)], axis=1
                ).astype(jnp.bfloat16)
                pieces.append(
                    lax.dot_general(
                        both, keys[index, :, k * wide : (k + 1) * wide],
                        (((1,), (1,)), ((), ())), preferred_element_type=jnp.float32,
                    )
                )
            scores = jnp.concatenate(pieces, axis=0) * HEAD_SIZE ** (-0.5)
            scored[d] = jnp.where(token < limit, scores, lowest)
        tops = {d: jnp.max(scored[d], axis=1, keepdims=True) for d in batch}
        weights = {d: jnp.exp(scored[d] - tops[d]) for d in batch}
        totals = {d: jnp.sum(weights[d], axis=1, keepdims=True) for d in batch}
        for d in batch:
            index, limit = homes[d]
            blocks = []
            for k in range(HQ // PAIR):
                w8 = weights[d][k * PAIR : (k + 1) * PAIR].astype(jnp.bfloat16)
                both = jnp.dot(
                    w8, values[index, :, k * wide : (k + 1) * wide], preferred_element_type=jnp.float32
                )
                blocks.append(jnp.where(first, both[:, :HEAD_SIZE], both[:, HEAD_SIZE:]))
            blocks.append(
                jnp.where(
                    sub8 == 0,
                    diagonal_to_lanes(tops[d], on_diagonal),
                    diagonal_to_lanes(totals[d], on_diagonal),
                )
            )
            block = jnp.concatenate(blocks, axis=0)
            if d == 0:
                part_in[my_req] = block
                continue
            part_send[d] = block
            copy = remote(part_send.at[d], part_in.at[my_req], ps_sem.at[0], pr_sem.at[0], (req_peers[d], my_kv))
            copy.start()
    arrived(part_in, n_req - 1, pr_sem.at[0])

    tops, totals = [], []
    for d in range(n_req):
        tops.append(part_in[req_peers[d], HQ : HQ + 1, :])
        totals.append(part_in[req_peers[d], HQ + 1 : HQ + 2, :])
    merged_top, merged_total = [], []
    factors = [jnp.zeros((1, HEAD_SIZE), jnp.float32) for _ in range(n_req)]
    member = [[jnp.broadcast_to(held[d], (1, HEAD_SIZE)) == float(c) for d in range(n_req)] for c in range(group)]
    for c in range(group):
        best = jnp.full((1, HEAD_SIZE), lowest, jnp.float32)
        for d in range(n_req):
            best = jnp.maximum(best, jnp.where(member[c][d], tops[d], lowest))
        merged_top.append(best)
    for d in range(n_req):
        best = tops[d]
        for c in range(group):
            best = jnp.where(member[c][d], merged_top[c], best)
        factors[d] = jnp.exp(tops[d] - best)
    for c in range(group):
        amount = jnp.zeros((1, HEAD_SIZE), jnp.float32)
        for d in range(n_req):
            amount = amount + jnp.where(member[c][d], factors[d] * totals[d], 0.0)
        merged_total.append(amount)
    sums = [jnp.zeros((HQ, HEAD_SIZE), jnp.float32) for _ in range(group)]
    for d in range(n_req):
        scaled = lanes_to_column(factors[d], on_diagonal) * part_in[req_peers[d], 0:HQ, :]
        pick = jnp.broadcast_to(held[d], (HQ, HEAD_SIZE))
        for c in range(group):
            sums[c] = sums[c] + jnp.where(pick == float(c), scaled, 0.0)
    for c in range(group):
        merged[c, 0:HQ, :] = sums[c]
        merged[c, HQ : HQ + STAT, :] = jnp.where(sub8 == 0, merged_top[c], merged_total[c])

    for d in range(n_kv - 1, 0, -1):
        copy = remote(merged.at[kv_peers[d]], merged_in.at[my_kv], ms_sem.at[0], mr_sem.at[0], (my_req, kv_peers[d]))
        copy.start()
    merged_in[my_kv] = merged[my_kv]
    arrived(merged_in, n_kv - 1, mr_sem.at[0])

    tops = [merged_in[c, HQ : HQ + 1, :] for c in range(n_kv)]
    best = tops[0]
    for c in range(1, n_kv):
        best = jnp.maximum(best, tops[c])
    factors = [jnp.exp(tops[c] - best) for c in range(n_kv)]
    amount = jnp.zeros((1, HEAD_SIZE), jnp.float32)
    for c in range(n_kv):
        amount = amount + factors[c] * merged_in[c, HQ + 1 : HQ + 2, :]
    result = jnp.zeros((HQ, HEAD_SIZE), jnp.float32)
    for c in range(n_kv):
        result = result + lanes_to_column(factors[c], on_diagonal) * merged_in[c, 0:HQ, :]
    result = result / lanes_to_column(amount, on_diagonal)
    out_ref[...] = result.astype(jnp.bfloat16)

    arrived(q_group, n_kv - 1, qs_sem.at[0])
    arrived(table, n_req - 1, ts_sem.at[0])
    arrived(q_send, n_req - 1, ds_sem.at[0])
    arrived(part_send, n_req - 1, ps_sem.at[0])
    arrived(merged, n_kv - 1, ms_sem.at[0])


def solution(mesh):
    n_req, n_kv = mesh.shape["req"], mesh.shape["kv"]

    def on_device(queries, key_cache, value_cache, page_request, page_number, lengths):
        slots, page_tokens, width = key_cache.shape
        group = lengths.shape[0] // n_req
        dma = pltpu.SemaphoreType.DMA
        vmem = pl.BlockSpec(memory_space=pltpu.VMEM)
        anywhere = pl.BlockSpec(memory_space=pl.ANY)
        blob = (HQ + STAT, HEAD_SIZE)
        attended = pl.pallas_call(
            functools.partial(kernel, n_req, n_kv, group),
            out_shape=pltpu.VMEM((HQ, HEAD_SIZE), jnp.bfloat16),
            in_specs=[anywhere] * 6,
            out_specs=vmem,
            scratch_shapes=[
                pltpu.SMEM(page_request.shape, jnp.int32),
                pltpu.SMEM(page_number.shape, jnp.int32),
                pltpu.SMEM(lengths.shape, jnp.int32),
                pltpu.VMEM(queries.shape, queries.dtype),
                pltpu.VMEM((slots, page_tokens, width), jnp.bfloat16),
                pltpu.VMEM((slots, page_tokens, width), jnp.bfloat16),
                pltpu.VMEM((HQ, HEAD_SIZE), jnp.float32),
                pltpu.VMEM((n_kv, HQ, HEAD_SIZE), jnp.bfloat16),
                pltpu.VMEM((n_req, STAT, HEAD_SIZE), jnp.float32),
                pltpu.VMEM((n_req, HQ, HEAD_SIZE), jnp.bfloat16),
                pltpu.VMEM((n_req, HQ, HEAD_SIZE), jnp.bfloat16),
                pltpu.VMEM((n_req,) + blob, jnp.float32),
                pltpu.VMEM((n_req,) + blob, jnp.float32),
                pltpu.VMEM((group,) + blob, jnp.float32),
                pltpu.VMEM((n_kv,) + blob, jnp.float32),
                dma((4,)),
                dma((2,)),
                dma((1,)), dma((1,)),
                dma((1,)), dma((1,)),
                dma((1,)), dma((3,)),
                dma((1,)), dma((1,)),
                dma((1,)), dma((1,)),
            ],
            compiler_params=pltpu.CompilerParams(collective_id=0, has_side_effects=True),
        )(page_request, page_number, lengths, queries, key_cache, value_cache)
        return attended.reshape(queries.shape)

    placed = (
        P(("req", "kv"), None),
        P(("req", "kv"), None, None),
        P(("req", "kv"), None, None),
        P(("req", "kv")),
        P(("req", "kv")),
        P(),
    )
    return jax.shard_map(
        on_device, mesh=mesh, in_specs=placed, out_specs=P(("req", "kv"), None), check_vma=False
    )
```

```python
import functools

import jax
import jax.numpy as jnp
from jax import lax
from jax.experimental import pallas as pl
from jax.experimental.pallas import tpu as pltpu
from jax.sharding import PartitionSpec as P

HQ = 32
KEY_VALUE_HEADS = 8
HEAD_SIZE = 128
QUERY_PER_KV = 4
PAIR = 2 * QUERY_PER_KV
STAT = 8

lowest = -1e30
MESH = pl.DeviceIdType.MESH


def partners(me, n):
    if n & (n - 1):
        return [lax.rem(me + d, n) for d in range(n)]
    found = []
    for d in range(n):
        place, bit = me, 1
        while bit < n:
            if d & bit:
                place = place + bit - 2 * bit * lax.rem(lax.div(me, bit), 2)
            bit *= 2
        found.append(place)
    return found


def diagonal_to_lanes(column, on_diagonal):
    return jnp.sum(jnp.where(on_diagonal, column, 0.0), axis=0, keepdims=True)


def lanes_to_column(row, on_diagonal):
    return jnp.sum(jnp.where(on_diagonal, row, 0.0), axis=1, keepdims=True)


def kernel(
    n_req, n_kv, group,
    owner_hbm, number_hbm, length_hbm, q_hbm, key_hbm, value_hbm, out_ref,
    owner_ref, number_ref, length_ref, q_ref, keys, values, q_rows, q_group, table, q_send, q_in, part_send, part_in, merged, merged_in,
    small_sem, page_sem, qs_sem, qr_sem, ts_sem, tr_sem, ds_sem, dr_sem, ps_sem, pr_sem, ms_sem, mr_sem,
):
    slots, page_tokens, _ = keys.shape
    my_req = lax.axis_index("req")
    my_kv = lax.axis_index("kv")

    barrier = pltpu.get_barrier_semaphore()
    req_peers = partners(my_req, n_req)
    kv_peers = partners(my_kv, n_kv)
    for d in range(n_kv - 1, 0, -1):
        pl.semaphore_signal(barrier, inc=1, device_id=(my_req, kv_peers[d]), device_id_type=MESH)
    for d in range(n_req - 1, 0, -1):
        pl.semaphore_signal(barrier, inc=1, device_id=(req_peers[d], my_kv), device_id_type=MESH)

    small = [
        pltpu.make_async_copy(src, dst, small_sem.at[i])
        for i, (src, dst) in enumerate(
            ((q_hbm, q_ref), (owner_hbm, owner_ref), (number_hbm, number_ref), (length_hbm, length_ref))
        )
    ]
    for copy in small:
        copy.start()

    loads = []
    for s in range(slots):
        loads.append(pltpu.make_async_copy(key_hbm.at[s], keys.at[s], page_sem.at[0]))
        loads.append(pltpu.make_async_copy(value_hbm.at[s], values.at[s], page_sem.at[1]))
    for load in loads:
        load.start()
    for copy in small:
        copy.wait()

    for h in range(HQ):
        q_rows[h : h + 1, :] = q_ref[0:1, h * HEAD_SIZE : (h + 1) * HEAD_SIZE].astype(jnp.float32)
    q_group[my_kv] = q_rows[...].astype(jnp.bfloat16)
    lane8 = lax.broadcasted_iota(jnp.int32, (STAT, HEAD_SIZE), 1)
    sub8 = lax.broadcasted_iota(jnp.int32, (STAT, HEAD_SIZE), 0)
    own_table = jnp.full((STAT, HEAD_SIZE), -1.0, jnp.float32)
    for s in range(slots):
        own_table = jnp.where(lane8 == s, owner_ref[s].astype(jnp.float32), own_table)
    table[my_req] = own_table

    pl.semaphore_wait(barrier, n_req - 1 + n_kv - 1)

    def remote(src, dst, send, recv, target):
        return pltpu.make_async_remote_copy(
            src_ref=src, dst_ref=dst, send_sem=send, recv_sem=recv,
            device_id=target, device_id_type=MESH,
        )

    def arrived(buffer, count, sem):
        if count:
            pltpu.make_async_copy(buffer.at[pl.ds(0, count)], buffer.at[pl.ds(0, count)], sem).wait()

    for d in range(n_kv - 1, 0, -1):
        copy = remote(q_group.at[my_kv], q_group.at[my_kv], qs_sem.at[0], qr_sem.at[0], (my_req, kv_peers[d]))
        copy.start()
    for d in range(n_req - 1, 0, -1):
        copy = remote(table.at[my_req], table.at[my_req], ts_sem.at[0], tr_sem.at[0], (req_peers[d], my_kv))
        copy.start()

    homes = []
    for d in range(n_req):
        index, present = jnp.int32(0), jnp.int32(0)
        for s in range(slots):
            same = lax.div(owner_ref[s], group) == req_peers[d]
            index = jnp.where(same, jnp.int32(s), index)
            present = jnp.where(same, jnp.int32(1), present)
        limit = length_ref[owner_ref[index]] - number_ref[index] * page_tokens
        homes.append((index, limit * present))

    arrived(table, n_req - 1, tr_sem.at[0])
    base = (my_req * group).astype(jnp.float32)
    held = []
    for d in range(n_req):
        rel = table[req_peers[d]] - base
        inside = jnp.logical_and(rel >= 0.0, rel < float(group))
        held.append(jnp.max(jnp.where(inside, rel, -1.0), axis=1, keepdims=True)[0:1])
    arrived(q_group, n_kv - 1, qr_sem.at[0])

    choices = [q_group[c].astype(jnp.float32) for c in range(group)]
    edges = [0, max(n_req // 4, 1), max(3 * n_req // 4, 1), n_req]
    stage_of = [sum(d >= edge for edge in edges[1:]) for d in range(n_req)]
    for d in list(range(n_req - 1, -1, -1)):
        pick = jnp.broadcast_to(held[d], (HQ, HEAD_SIZE))
        chosen = jnp.zeros((HQ, HEAD_SIZE), jnp.float32)
        for c in range(group):
            chosen = jnp.where(pick == float(c), choices[c], chosen)
        if d == 0:
            q_in[my_req] = chosen.astype(jnp.bfloat16)
            continue
        q_send[d] = chosen.astype(jnp.bfloat16)
        copy = remote(q_send.at[d], q_in.at[my_req], ds_sem.at[0], dr_sem.at[stage_of[d]], (req_peers[d], my_kv))
        copy.start()

    pltpu.make_async_copy(key_hbm, keys, page_sem.at[0]).wait()
    pltpu.make_async_copy(value_hbm, values, page_sem.at[1]).wait()

    row = lax.broadcasted_iota(jnp.int32, (HQ, HEAD_SIZE), 0)
    lane = lax.broadcasted_iota(jnp.int32, (HQ, HEAD_SIZE), 1)
    on_diagonal = row == lane
    first = sub8 < QUERY_PER_KV
    token = lax.broadcasted_iota(jnp.int32, (HQ, page_tokens), 1)
    wide = 2 * HEAD_SIZE

    for stage, (low, high) in enumerate(zip(edges[:-1], edges[1:])):
        batch = range(high - 1, low - 1, -1)
        arrived(q_in, high - max(low, 1), dr_sem.at[stage])
        scored = {}
        for d in batch:
            index, limit = homes[d]
            query = q_in[req_peers[d]].astype(jnp.float32)
            pieces = []
            for k in range(HQ // PAIR):
                q8 = query[k * PAIR : (k + 1) * PAIR]
                both = jnp.concatenate(
                    [jnp.where(first, q8, 0.0), jnp.where(first, 0.0, q8)], axis=1
                ).astype(jnp.bfloat16)
                pieces.append(
                    lax.dot_general(
                        both, keys[index, :, k * wide : (k + 1) * wide],
                        (((1,), (1,)), ((), ())), preferred_element_type=jnp.float32,
                    )
                )
            scores = jnp.concatenate(pieces, axis=0) * HEAD_SIZE ** (-0.5)
            scored[d] = jnp.where(token < limit, scores, lowest)
        tops = {d: jnp.max(scored[d], axis=1, keepdims=True) for d in batch}
        weights = {d: jnp.exp(scored[d] - tops[d]) for d in batch}
        totals = {d: jnp.sum(weights[d], axis=1, keepdims=True) for d in batch}
        for d in batch:
            index, limit = homes[d]
            blocks = []
            for k in range(HQ // PAIR):
                w8 = weights[d][k * PAIR : (k + 1) * PAIR].astype(jnp.bfloat16)
                both = jnp.dot(
                    w8, values[index, :, k * wide : (k + 1) * wide], preferred_element_type=jnp.float32
                )
                blocks.append(jnp.where(first, both[:, :HEAD_SIZE], both[:, HEAD_SIZE:]))
            blocks.append(diagonal_to_lanes(tops[d], on_diagonal))
            blocks.append(diagonal_to_lanes(totals[d], on_diagonal))
            block = jnp.concatenate(blocks, axis=0)
            if d == 0:
                part_in[my_req] = block
                continue
            part_send[d] = block
            copy = remote(part_send.at[d], part_in.at[my_req], ps_sem.at[0], pr_sem.at[0], (req_peers[d], my_kv))
            copy.start()
    arrived(part_in, n_req - 1, pr_sem.at[0])

    tops, totals = [], []
    for d in range(n_req):
        tops.append(part_in[req_peers[d], HQ : HQ + 1, :])
        totals.append(part_in[req_peers[d], HQ + 1 : HQ + 2, :])
    merged_top, merged_total = [], []
    factors = [jnp.zeros((1, HEAD_SIZE), jnp.float32) for _ in range(n_req)]
    member = [[jnp.broadcast_to(held[d], (1, HEAD_SIZE)) == float(c) for d in range(n_req)] for c in range(group)]
    for c in range(group):
        best = jnp.full((1, HEAD_SIZE), lowest, jnp.float32)
        for d in range(n_req):
            best = jnp.maximum(best, jnp.where(member[c][d], tops[d], lowest))
        merged_top.append(best)
    for d in range(n_req):
        best = tops[d]
        for c in range(group):
            best = jnp.where(member[c][d], merged_top[c], best)
        factors[d] = jnp.exp(tops[d] - best)
    for c in range(group):
        amount = jnp.zeros((1, HEAD_SIZE), jnp.float32)
        for d in range(n_req):
            amount = amount + jnp.where(member[c][d], factors[d] * totals[d], 0.0)
        merged_total.append(amount)
    sums = [jnp.zeros((HQ, HEAD_SIZE), jnp.float32) for _ in range(group)]
    for d in range(n_req):
        scaled = lanes_to_column(factors[d], on_diagonal) * part_in[req_peers[d], 0:HQ, :]
        pick = jnp.broadcast_to(held[d], (HQ, HEAD_SIZE))
        for c in range(group):
            sums[c] = sums[c] + jnp.where(pick == float(c), scaled, 0.0)
    for c in range(group):
        merged[c, 0:HQ, :] = sums[c]
        merged[c, HQ : HQ + 2, :] = jnp.concatenate([merged_top[c], merged_total[c]], axis=0)

    for d in range(n_kv - 1, 0, -1):
        copy = remote(merged.at[kv_peers[d]], merged_in.at[my_kv], ms_sem.at[0], mr_sem.at[0], (my_req, kv_peers[d]))
        copy.start()
    merged_in[my_kv] = merged[my_kv]
    arrived(merged_in, n_kv - 1, mr_sem.at[0])

    tops = [merged_in[c, HQ : HQ + 1, :] for c in range(n_kv)]
    best = tops[0]
    for c in range(1, n_kv):
        best = jnp.maximum(best, tops[c])
    factors = [jnp.exp(tops[c] - best) for c in range(n_kv)]
    amount = jnp.zeros((1, HEAD_SIZE), jnp.float32)
    for c in range(n_kv):
        amount = amount + factors[c] * merged_in[c, HQ + 1 : HQ + 2, :]
    result = jnp.zeros((HQ, HEAD_SIZE), jnp.float32)
    for c in range(n_kv):
        result = result + lanes_to_column(factors[c], on_diagonal) * merged_in[c, 0:HQ, :]
    result = result / lanes_to_column(amount, on_diagonal)
    out_ref[...] = result.astype(jnp.bfloat16)

    arrived(q_group, n_kv - 1, qs_sem.at[0])
    arrived(table, n_req - 1, ts_sem.at[0])
    arrived(q_send, n_req - 1, ds_sem.at[0])
    arrived(part_send, n_req - 1, ps_sem.at[0])
    arrived(merged, n_kv - 1, ms_sem.at[0])


def solution(mesh):
    n_req, n_kv = mesh.shape["req"], mesh.shape["kv"]

    def on_device(queries, key_cache, value_cache, page_request, page_number, lengths):
        slots, page_tokens, width = key_cache.shape
        group = lengths.shape[0] // n_req
        dma = pltpu.SemaphoreType.DMA
        vmem = pl.BlockSpec(memory_space=pltpu.VMEM)
        anywhere = pl.BlockSpec(memory_space=pl.ANY)
        blob = (HQ + 2, HEAD_SIZE)
        attended = pl.pallas_call(
            functools.partial(kernel, n_req, n_kv, group),
            out_shape=pltpu.VMEM((HQ, HEAD_SIZE), jnp.bfloat16),
            in_specs=[anywhere] * 6,
            out_specs=vmem,
            scratch_shapes=[
                pltpu.SMEM(page_request.shape, jnp.int32),
                pltpu.SMEM(page_number.shape, jnp.int32),
                pltpu.SMEM(lengths.shape, jnp.int32),
                pltpu.VMEM(queries.shape, queries.dtype),
                pltpu.VMEM((slots, page_tokens, width), jnp.bfloat16),
                pltpu.VMEM((slots, page_tokens, width), jnp.bfloat16),
                pltpu.VMEM((HQ, HEAD_SIZE), jnp.float32),
                pltpu.VMEM((n_kv, HQ, HEAD_SIZE), jnp.bfloat16),
                pltpu.VMEM((n_req, STAT, HEAD_SIZE), jnp.float32),
                pltpu.VMEM((n_req, HQ, HEAD_SIZE), jnp.bfloat16),
                pltpu.VMEM((n_req, HQ, HEAD_SIZE), jnp.bfloat16),
                pltpu.VMEM((n_req,) + blob, jnp.float32),
                pltpu.VMEM((n_req,) + blob, jnp.float32),
                pltpu.VMEM((group,) + blob, jnp.float32),
                pltpu.VMEM((n_kv,) + blob, jnp.float32),
                dma((4,)),
                dma((2,)),
                dma((1,)), dma((1,)),
                dma((1,)), dma((1,)),
                dma((1,)), dma((3,)),
                dma((1,)), dma((1,)),
                dma((1,)), dma((1,)),
            ],
            compiler_params=pltpu.CompilerParams(collective_id=0, has_side_effects=True),
        )(page_request, page_number, lengths, queries, key_cache, value_cache)
        return attended.reshape(queries.shape)

    placed = (
        P(("req", "kv"), None),
        P(("req", "kv"), None, None),
        P(("req", "kv"), None, None),
        P(("req", "kv")),
        P(("req", "kv")),
        P(),
    )
    return jax.shard_map(
        on_device, mesh=mesh, in_specs=placed, out_specs=P(("req", "kv"), None), check_vma=False
    )
```
